32 devices in a mesh: dp: 16 (over z, y, x), head: 2 (over core).
Axes of the slice: x: 2, y: 2, z: 4, core: 2. Of those that a mesh axis runs over, the one named last changes fastest.
Arguments:
- teacher_hidden: bfloat16 [40960, 1024], P('dp', 'head'), may hold values from -6 to 6
- student_hidden: bfloat16 [40960, 312], P('dp'), may hold values from -6 to 6
- projector: bfloat16 [312, 1024], P(None, 'head'), may hold values from -0.3125 to 0.3125
- teacher_queries: bfloat16 [40960, 1024], P('dp', 'head'), may hold values from -6 to 6
- teacher_keys: bfloat16 [40960, 1024], P('dp', 'head'), may hold values from -6 to 6
- student_queries: bfloat16 [40960, 312], P('dp', 'head'), may hold values from -6 to 6
- student_keys: bfloat16 [40960, 312], P('dp', 'head'), may hold values from -6 to 6
- lengths: int32 [80], replicated, may hold values from 32 to 512, as said below
- plan: int32 [4, 16], replicated, may hold values from 0 to 4, as said below
Outputs:
- hidden_row: float32 [40960], P(('dp', 'head'))
- row_loss: float32 [16, 2, 5, 256], P('dp', 'head')
- loss: float32 [], replicated
The draws below stay inside these ranges and needn't reach their ends.
Inputs may be any that keep to these rules, and one draw needn't show every extreme that they name: lengths[k] counts the real tokens of the sequence in rows k * 512 onward, first held in slot k mod 5 of dp index k // 5; the rows after them are padding. Some sequence has exactly 512 tokens. In round r, dp index d gives the sequence in its slot plan[r, d] to dp index d XOR 2^r and receives that device's slot plan[r, d XOR 2^r] into the same slot; the rounds tend to even out the sum of squared lengths of the devices.
All inputs are finite; a program needn't handle non-finite values.
Results may differ from the reference program's by a relative error of at most 0.0003.
Values may be sent and summed in bfloat16 or wider, within the bound.
A program may use at most 128 MiB of HBM per device.

```python
import math
import jax
import jax.numpy as jnp
from jax import lax

HEADS_T = 16
HEAD_T = 64
HEADS_S = 12
HEAD_S = 26
MAXLEN = 512
SEQ_DEV = 5
D_T = 1024
D_S = 312
SEQS = 80
ROWS = 40960
ROUNDS = 4
N_HEAD = 2


def partner_rows_drawn(values, bit_index):
    block_span = 2 ** bit_index
    total_rows = values.shape[0]
    grouped = values.reshape((total_rows // (2 * block_span), 2, block_span) + values.shape[1:])
    return grouped[:, ::-1].reshape(values.shape)


def swap_slots_drawn(slot_table, chosen, bit_index):
    slot_order = jnp.arange(slot_table.shape[1], dtype=jnp.int32)
    partner_vals = partner_rows_drawn(slot_table, bit_index)
    partner_slot = partner_rows_drawn(chosen, bit_index)
    incoming = jnp.sum(jnp.where(slot_order[None, :] == partner_slot[:, None], partner_vals, 0), axis=1).astype(jnp.int32)
    return jnp.where(slot_order[None, :] == chosen[:, None], incoming[:, None], slot_table).astype(jnp.int32)


def shared_lengths(key):
    base_key = jax.random.fold_in(key, 7)
    shortest = MAXLEN // 16
    drawn_lengths = jax.random.randint(jax.random.fold_in(base_key, 1), (SEQS,), shortest, MAXLEN + 1, dtype=jnp.int32)
    marked = jax.random.permutation(jax.random.fold_in(base_key, 2), SEQS)
    positions = jnp.arange(SEQS, dtype=jnp.int32)
    drawn_lengths = jnp.where(positions == marked[0], MAXLEN, drawn_lengths)
    return jnp.where(positions == marked[1], shortest, drawn_lengths).astype(jnp.int32)


def draw_lengths(key, part):
    return shared_lengths(key)


def draw_plan(key, part):
    device_count = SEQS // SEQ_DEV
    slot_table = shared_lengths(key).reshape(device_count, SEQ_DEV)
    slot_order = jnp.arange(SEQ_DEV, dtype=jnp.int32)
    identity = jnp.arange(device_count, dtype=jnp.int32)
    chosen_rows = []
    for bit_index in range(ROUNDS):
        squares = slot_table * slot_table
        work_load = jnp.sum(squares, axis=1).astype(jnp.int32)
        partner_load = partner_rows_drawn(work_load, bit_index)
        partner_id = partner_rows_drawn(identity, bit_index)
        heavier = (work_load > partner_load) | (work_load == partner_load) & (identity > partner_id)
        longest = jnp.argmax(slot_table * SEQ_DEV + slot_order[None, :], axis=1).astype(jnp.int32)
        partner_big = partner_rows_drawn(jnp.max(squares, axis=1), bit_index)
        imbalance = jnp.abs(partner_load[:, None] - work_load[:, None] - 2 * partner_big[:, None] + 2 * squares)
        lightest = jnp.argmin(imbalance * SEQ_DEV + slot_order[None, :], axis=1).astype(jnp.int32)
        chosen = jnp.where(heavier, longest, lightest).astype(jnp.int32)
        chosen_rows.append(chosen)
        slot_table = swap_slots_drawn(slot_table, chosen, bit_index)
    return jnp.stack(chosen_rows).astype(jnp.int32)


def shard_levels(key, dims, split, low, high):
    def one(position, parts):
        steps = jax.random.uniform(jax.random.fold_in(jax.random.fold_in(key, 6), position), (parts,), jnp.float32, low / len(split), high / len(split))
        return jnp.repeat(jnp.exp(steps), dims[position] // parts).reshape((-1,) + (1,) * (len(dims) - position - 1))

    level = one(*split[0])
    for cut in split[1:]:
        level = level * one(*cut)
    return level


def scatter_about(own_key, dims, scale, reach, cuts=(), kind=jnp.bfloat16):
    entries = jax.random.normal(own_key, dims, jnp.float32) * scale
    if len(cuts) > 0:
        entries = shard_levels(own_key, dims, cuts, -0.22, 0.18) * entries
    return jnp.clip(entries, min=-reach, max=reach).astype(kind)


def setup_inputs(seed: int = 0) -> dict:
    key_list = jax.random.split(jax.random.key(seed), 10)
    teacher_hidden = scatter_about(key_list[0], (ROWS, D_T), 1.0, 6.0, ((0, 16), (1, 2)))
    student_hidden = scatter_about(key_list[1], (ROWS, D_S), 1.0, 6.0, ((0, 16),))
    projector = scatter_about(key_list[2], (D_S, D_T), D_S ** -0.5, 0.3125, ((1, 2),))
    teacher_queries = scatter_about(key_list[3], (ROWS, D_T), 1.0, 6.0, ((0, 16), (1, 2)))
    teacher_keys = scatter_about(key_list[4], (ROWS, D_T), 1.0, 6.0, ((0, 16), (1, 2)))
    student_queries = scatter_about(key_list[5], (ROWS, D_S), 1.0, 6.0, ((0, 16), (1, 2)))
    student_keys = scatter_about(key_list[6], (ROWS, D_S), 1.0, 6.0, ((0, 16), (1, 2)))
    lengths = draw_lengths(jax.random.fold_in(key_list[9], 71), 0)
    plan = draw_plan(jax.random.fold_in(key_list[9], 71), 0)
    return {"teacher_hidden": teacher_hidden, "student_hidden": student_hidden, "projector": projector, "teacher_queries": teacher_queries, "teacher_keys": teacher_keys, "student_queries": student_queries, "student_keys": student_keys, "lengths": lengths, "plan": plan}


def partner_rows(values, bit_index):
    block_span = 2 ** bit_index
    total_rows = values.shape[0]
    grouped = values.reshape((total_rows // (2 * block_span), 2, block_span) + values.shape[1:])
    return grouped[:, ::-1].reshape(values.shape)

def swap_slots(slot_table, chosen, bit_index):
    slot_order = jnp.arange(slot_table.shape[1], dtype=jnp.int32)
    partner_vals = partner_rows(slot_table, bit_index)
    partner_slot = partner_rows(chosen, bit_index)
    incoming = lax.optimization_barrier(jnp.sum(jnp.where(slot_order[None, :] == partner_slot[:, None], partner_vals, 0), axis=1)).astype(jnp.int32)
    return jnp.where(slot_order[None, :] == chosen[:, None], incoming[:, None], slot_table).astype(jnp.int32)

def reference(teacher_hidden, student_hidden, projector, teacher_queries, teacher_keys, student_queries, student_keys, lengths, plan):
    t_scale = 1.0 / (HEADS_T * math.sqrt(HEAD_T))
    s_scale = 1.0 / (HEADS_S * math.sqrt(HEAD_S))
    device_count = plan.shape[1]
    owner_table = jnp.arange(SEQS, dtype=jnp.int32).reshape(device_count, SEQ_DEV)
    for bit_index in range(plan.shape[0]):
        owner_table = swap_slots(owner_table, plan[bit_index].astype(jnp.int32), bit_index)
    positions = jnp.arange(MAXLEN, dtype=jnp.int32)

    def hidden_one(seq_index):
        row_start = (seq_index * MAXLEN).astype(jnp.int32)
        student = lax.dynamic_slice_in_dim(student_hidden, row_start, MAXLEN, 0)
        teacher = lax.dynamic_slice_in_dim(teacher_hidden, row_start, MAXLEN, 0).astype(jnp.float32)
        projected = jnp.dot(student, projector, preferred_element_type=jnp.float32)
        errors = lax.optimization_barrier(jnp.sum((projected - teacher) * (projected - teacher), axis=1)) / D_T
        return jnp.where(positions < lengths[seq_index], errors, 0.0)
    hidden_row = lax.map(hidden_one, jnp.arange(SEQS, dtype=jnp.int32)).reshape(ROWS)

    def attend_one(seq_index):
        row_start = (seq_index * MAXLEN).astype(jnp.int32)
        t_query = lax.dynamic_slice_in_dim(teacher_queries, row_start, MAXLEN, 0)
        t_key = lax.dynamic_slice_in_dim(teacher_keys, row_start, MAXLEN, 0)
        s_query = lax.dynamic_slice_in_dim(student_queries, row_start, MAXLEN, 0)
        s_key = lax.dynamic_slice_in_dim(student_keys, row_start, MAXLEN, 0)
        teacher_map = jnp.dot(t_query, t_key.T, preferred_element_type=jnp.float32)
        student_map = jnp.dot(s_query, s_key.T, preferred_element_type=jnp.float32)
        length = lengths[seq_index]
        inside = positions < length
        difference = jnp.where(inside[:, None] & inside[None, :], teacher_map * t_scale - student_map * s_scale, 0.0)
        squares = difference * difference
        return (lax.optimization_barrier(jnp.sum(squares, axis=1)) / length.astype(jnp.float32), jnp.sum(squares))
    per_row, seq_totals = lax.map(attend_one, owner_table.reshape(SEQS))
    row_loss = per_row.reshape(device_count, SEQ_DEV, N_HEAD, MAXLEN // N_HEAD).transpose(0, 2, 1, 3)
    lengths_float = lengths.astype(jnp.float32)
    loss = jnp.sum(hidden_row) / jnp.sum(lengths_float) + jnp.sum(seq_totals) / jnp.sum(lengths_float * lengths_float)
    return (hidden_row, row_loss, loss)
```

```python
import functools
import math

import jax
import jax.numpy as jnp
from jax import lax
from jax.experimental import pallas as pl
from jax.experimental.pallas import tpu as pltpu
from jax.sharding import PartitionSpec as P

HEADS_T = 16
HEAD_T = 64
HEADS_S = 12
HEAD_S = 26
MESH = pl.DeviceIdType.MESH
NT = (((1,), (1,)), ((), ()))


def kernel(
    device_count, slots, rounds, width,
    th, sh, pj, tq, tk, sq, sk, lens, plan,
    hid_out, row_out, loss_out,
    thv, shv, pjv, tqv, tkv, sqv, skv,
    send, own, recv, hpart, hrecv, gath, tots,
    in_sem, pj_sem, x_send, x_recv, h_send, h_recv, g_send, g_recv, t_send, t_recv,
):
    me = lax.axis_index("dp")
    head = lax.axis_index("head")
    other = 1 - head
    tokens = tqv.shape[1]
    half = tokens // 2
    t_scale = 1.0 / (HEADS_T * math.sqrt(HEAD_T))
    s_scale = 1.0 / (HEADS_S * math.sqrt(HEAD_S))

    def fetch(index, source, target, slot):
        return pltpu.make_async_copy(
            source.at[pl.ds(slot * tokens, tokens), :], target.at[slot], in_sem.at[index, slot]
        )

    attend = ((tk, tkv), (tq, tqv), (sk, skv), (sq, sqv))
    hidden = ((sh, shv), (th, thv))

    @pl.loop(0, slots)
    def _(slot):
        for index, (source, target) in enumerate(attend):
            fetch(index, source, target, slot).start()

    pltpu.make_async_copy(pj, pjv, pj_sem).start()

    @pl.loop(0, slots)
    def _(slot):
        for index, (source, target) in enumerate(hidden):
            fetch(4 + index, source, target, slot).start()

    barrier = pltpu.get_barrier_semaphore()
    pl.semaphore_signal(barrier, inc=1, device_id=(me, other), device_id_type=MESH)

    @pl.loop(1, device_count)
    def _(step):
        peer = lax.rem(me + step, device_count)
        pl.semaphore_signal(barrier, inc=1, device_id=(peer, head), device_id_type=MESH)
        pl.semaphore_signal(barrier, inc=1, device_id=(peer, other), device_id_type=MESH)

    def exchange(slot):
        return pltpu.make_async_remote_copy(
            src_ref=send.at[slot], dst_ref=recv.at[slot],
            send_sem=x_send.at[slot], recv_sem=x_recv.at[slot],
            device_id=(me, other), device_id_type=MESH,
        )

    @pl.loop(0, slots)
    def _(slot):
        for index, (source, target) in enumerate(attend):
            fetch(index, source, target, slot).wait()

        def scores(which):
            rows = pl.ds(pl.multiple_of(which * half, half), half)
            teach = lax.dot_general(
                tkv[slot], tqv[slot, rows, :], NT, preferred_element_type=jnp.float32
            )
            pupil = lax.dot_general(
                skv[slot], sqv[slot, rows, :], NT, preferred_element_type=jnp.float32
            )
            return teach - pupil * (s_scale / t_scale)

        send[slot] = scores(other)
        own[slot] = scores(head)

        @pl.when(slot == 0)
        def _():
            pl.semaphore_wait(barrier, 2 * device_count - 1)

        exchange(slot).start()

    pltpu.make_async_copy(pj, pjv, pj_sem).wait()
    lanes = lax.broadcasted_iota(jnp.int32, (1, tokens), 1)

    @pl.loop(0, slots)
    def _(slot):
        for index, (source, target) in enumerate(hidden):
            fetch(4 + index, source, target, slot).wait()
        projected = jnp.dot(shv[slot], pjv[...], preferred_element_type=jnp.float32)
        errors = projected - thv[slot].astype(jnp.float32)
        squares = errors * errors
        folded = squares[:, :128]
        for start in range(128, squares.shape[1], 128):
            folded = folded + squares[:, start : start + 128]
        sums = jnp.sum(folded.T, axis=0, keepdims=True)
        sums = jnp.where(lanes < lens[me * slots + slot], sums, 0.0)
        hpart[2 * slot] = sums[:, :half]
        hpart[2 * slot + 1] = sums[:, half:]

    def add_length(index, sums):
        length = lens[index]
        return sums[0] + length, sums[1] + length * length

    total, total_sq = lax.fori_loop(
        0, device_count * slots, add_length, (jnp.int32(0), jnp.int32(0)), unroll=slots
    )

    owners = []
    for slot in range(slots):
        device, place = me, jnp.int32(slot)
        for bit in reversed(range(rounds)):
            mate = device ^ (2**bit)
            gave = plan[bit, device] == place
            place = jnp.where(gave, plan[bit, mate], place)
            device = jnp.where(gave, mate, device)
        owners.append((device, place))

    hidden_copy = pltpu.make_async_remote_copy(
        src_ref=hpart.at[pl.ds(other * slots, slots)], dst_ref=hrecv,
        send_sem=h_send, recv_sem=h_recv,
        device_id=(me, other), device_id_type=MESH,
    )
    hidden_copy.start()

    queries = lax.broadcasted_iota(jnp.int32, (1, half), 1) + head * half

    def reduce_slot(slot, totals):
        exchange(slot).wait_recv()
        length = lens[me * slots + slot]
        difference = own[slot] + recv[slot]
        keys = lax.broadcasted_iota(jnp.int32, (tokens, half), 0)
        squares = jnp.where(keys < length, difference * difference, 0.0)
        sums = jnp.sum(squares, axis=0, keepdims=True)
        sums = jnp.where(queries < length, sums * (t_scale * t_scale), 0.0)
        gath[me, slot] = sums / length.astype(jnp.float32)
        return totals + sums

    attention = lax.fori_loop(0, slots, reduce_slot, jnp.zeros((1, half), jnp.float32))

    hidden_copy.wait_recv()
    hidden_sum = jnp.zeros((1, half), jnp.float32)
    for row in range(slots):
        value = (hpart[head * slots + row] + hrecv[row]) / width
        for part in range(half // 128):
            index = row * (half // 128) + part
            hid_out[index : index + 1, :] = value[:, part * 128 : (part + 1) * 128]
        hidden_sum = hidden_sum + value
    gath[me, slots] = hidden_sum / total.astype(jnp.float32) + attention / total_sq.astype(
        jnp.float32
    )

    def rows_copy(step, source):
        return pltpu.make_async_remote_copy(
            src_ref=gath.at[source], dst_ref=gath.at[source],
            send_sem=g_send.at[step], recv_sem=g_recv.at[step],
            device_id=(lax.rem(me + step, device_count), head), device_id_type=MESH,
        )

    def total_copy(step, source):
        return pltpu.make_async_remote_copy(
            src_ref=gath.at[source, slots], dst_ref=tots.at[source],
            send_sem=t_send.at[step], recv_sem=t_recv.at[step],
            device_id=(lax.rem(me + step, device_count), other), device_id_type=MESH,
        )

    @pl.loop(1, device_count)
    def _(step):
        rows_copy(step, me).start()
        total_copy(step, me).start()

    total_copy(0, me).start()

    @pl.loop(0, slots)
    def _(slot):
        exchange(slot).wait_send()

    hidden_copy.wait_send()
    total_copy(0, me).wait_recv()

    @pl.loop(1, device_count)
    def _(step):
        source = lax.rem(me + device_count - step, device_count)
        rows_copy(step, source).wait_recv()
        total_copy(step, source).wait_recv()

    for slot, (device, place) in enumerate(owners):
        row_out[slot : slot + 1, :] = gath[device, place]
    pieces = jnp.sum(gath[:, slots], axis=0) + jnp.sum(tots[...], axis=0)
    loss_out[0, 0] = jnp.sum(pieces)

    total_copy(0, me).wait_send()

    @pl.loop(1, device_count)
    def _(step):
        rows_copy(step, me).wait_send()
        total_copy(step, me).wait_send()


def body(device_count, width, *operands):
    teacher_hidden, student_hidden, projector, _, _, student_queries, _, lengths, plan = operands
    slots = lengths.shape[0] // device_count
    tokens = teacher_hidden.shape[0] // slots
    half = tokens // 2
    cols_t = teacher_hidden.shape[1]
    cols_h = student_hidden.shape[1]
    cols_s = student_queries.shape[1]
    bf16, f32 = jnp.bfloat16, jnp.float32
    dma = pltpu.SemaphoreType.DMA
    anywhere = pl.BlockSpec(memory_space=pl.ANY)
    smem = pl.BlockSpec(memory_space=pltpu.SMEM)
    vmem = pl.BlockSpec(memory_space=pltpu.VMEM)
    hidden_row, row_loss, loss = pl.pallas_call(
        functools.partial(kernel, device_count, slots, plan.shape[0], width),
        out_shape=(
            jax.ShapeDtypeStruct((slots * half // 128, 128), f32),
            jax.ShapeDtypeStruct((slots, half), f32),
            jax.ShapeDtypeStruct((1, 1), f32),
        ),
        in_specs=[anywhere] * 7 + [smem] * 2,
        out_specs=(vmem, vmem, smem),
        scratch_shapes=[
            pltpu.VMEM((slots, tokens, cols_t), bf16),
            pltpu.VMEM((slots, tokens, cols_h), bf16),
            pltpu.VMEM(projector.shape, bf16),
            pltpu.VMEM((slots, tokens, cols_t), bf16),
            pltpu.VMEM((slots, tokens, cols_t), bf16),
            pltpu.VMEM((slots, tokens, cols_s), bf16),
            pltpu.VMEM((slots, tokens, cols_s), bf16),
            pltpu.VMEM((slots, tokens, half), f32),
            pltpu.VMEM((slots, tokens, half), f32),
            pltpu.VMEM((slots, tokens, half), f32),
            pltpu.VMEM((2 * slots, 1, half), f32),
            pltpu.VMEM((slots, 1, half), f32),
            pltpu.VMEM((device_count, slots + 1, 1, half), f32),
            pltpu.VMEM((device_count, 1, half), f32),
            dma((6, slots)),
            dma,
            dma((slots,)),
            dma((slots,)),
            dma,
            dma,
            dma((device_count,)),
            dma((device_count,)),
            dma((device_count,)),
            dma((device_count,)),
        ],
        compiler_params=pltpu.CompilerParams(
            collective_id=0, has_side_effects=True, vmem_limit_bytes=60 * 1024 * 1024
        ),
    )(*operands)
    return (
        hidden_row.reshape(slots * half),
        row_loss.reshape(1, 1, slots, half),
        loss.reshape(()),
    )


def solution(mesh):
    placed = (
        P("dp", "head"),
        P("dp", None),
        P(None, "head"),
        P("dp", "head"),
        P("dp", "head"),
        P("dp", "head"),
        P("dp", "head"),
        P(),
        P(),
    )

    def whole(*operands):
        width = operands[0].shape[1]
        return jax.shard_map(
            functools.partial(body, mesh.shape["dp"], width),
            mesh=mesh,
            in_specs=placed,
            out_specs=(P(("dp", "head")), P("dp", "head", None, None), P()),
            check_vma=False,
        )(*operands)

    return whole
```

```python
import functools
import math

import jax
import jax.numpy as jnp
from jax import lax
from jax.experimental import pallas as pl
from jax.experimental.pallas import tpu as pltpu
from jax.sharding import PartitionSpec as P

HEADS_T = 16
HEAD_T = 64
HEADS_S = 12
HEAD_S = 26
MESH = pl.DeviceIdType.MESH
NT = (((1,), (1,)), ((), ()))
TN = (((0,), (0,)), ((), ()))


def kernel(
    device_count, slots, rounds, width,
    th, sh, pj, tq, tk, sq, sk, lens_hbm, plan_hbm,
    hid_out, row_out, loss_out,
    thv, shv, pjv, tqv, tkv, sqv, skv,
    lens, plan, totalv, send, own, recv, hpart, hrecv, gath, tots,
    in_sem, pj_sem, x_send, x_recv, h_send, h_recv, g_send, g_recv, t_send, t_recv, s_sem,
):
    me = lax.axis_index("dp")
    head = lax.axis_index("head")
    other = 1 - head
    tokens = tqv.shape[1]
    half = tokens // 2
    t_scale = 1.0 / (HEADS_T * math.sqrt(HEAD_T))
    s_scale = 1.0 / (HEADS_S * math.sqrt(HEAD_S))

    def fetch(index, source, target, slot):
        span = pl.ds(pl.multiple_of(slot * tokens, tokens), tokens)
        piece = source.at[:, span] if index in (2, 3, 4) else source.at[span, :]
        return pltpu.make_async_copy(piece, target.at[slot], in_sem.at[index, slot])

    attend = ((tk, tkv), (tq, tqv), (sk, skv), (sq, sqv))
    hidden = ((sh, shv), (th, thv))

    scalars = (
        pltpu.make_async_copy(lens_hbm, lens, s_sem.at[0]),
        pltpu.make_async_copy(plan_hbm, plan, s_sem.at[1]),
    )
    for copy in scalars:
        copy.start()
    for index, (source, target) in enumerate(attend):
        fetch(index, source, target, 0).start()

    barrier = pltpu.get_barrier_semaphore()
    pl.semaphore_signal(barrier, inc=1, device_id=(me, other), device_id_type=MESH)

    @pl.loop(1, device_count)
    def _(step):
        peer = lax.rem(me + step, device_count)
        pl.semaphore_signal(barrier, inc=1, device_id=(peer, head), device_id_type=MESH)
        pl.semaphore_signal(barrier, inc=1, device_id=(peer, other), device_id_type=MESH)

    @pl.loop(1, slots)
    def _(slot):
        for index, (source, target) in enumerate(attend):
            fetch(index, source, target, slot).start()

    pltpu.make_async_copy(pj, pjv, pj_sem).start()

    @pl.loop(0, slots)
    def _(slot):
        for index, (source, target) in enumerate(hidden):
            fetch(4 + index, source, target, slot).start()

    for copy in scalars:
        copy.wait()

    def add_length(index, sums):
        length = lens[index]
        return sums[0] + length, sums[1] + length * length

    total, total_sq = lax.fori_loop(
        0, device_count * slots, add_length, (jnp.int32(0), jnp.int32(0)), unroll=slots
    )

    owners = []
    for slot in range(slots):
        device, place = me, jnp.int32(slot)
        for bit in reversed(range(rounds)):
            mate = device ^ (2**bit)
            gave = plan[bit, device] == place
            place = jnp.where(gave, plan[bit, mate], place)
            device = jnp.where(gave, mate, device)
        owners.append((device, place))

    gate = min(2, slots - 1)

    def exchange(slot):
        return pltpu.make_async_remote_copy(
            src_ref=send.at[slot], dst_ref=recv.at[slot],
            send_sem=x_send, recv_sem=x_recv.at[slot],
            device_id=(me, other), device_id_type=MESH,
        )

    @pl.loop(0, slots)
    def _(slot):
        for index, (source, target) in enumerate(attend):
            fetch(index, source, target, slot).wait()

        def scores(which):
            rows = pl.ds(pl.multiple_of(which * half, half), half)
            teach = lax.dot_general(
                tkv[slot], tqv[slot, rows, :], NT, preferred_element_type=jnp.float32
            )
            pupil = lax.dot_general(
                skv[slot], sqv[slot, :, rows], TN, preferred_element_type=jnp.float32
            )
            return teach - pupil * (s_scale / t_scale)

        send[slot] = scores(other)
        own[slot] = scores(head)

        @pl.when(slot == gate)
        def _():
            pl.semaphore_wait(barrier, 2 * device_count - 1)

            @pl.loop(0, gate)
            def _(done):
                exchange(done).start()

        @pl.when(slot >= gate)
        def _():
            exchange(slot).start()

    def rows_copy(step):
        rows = gath.at[me]
        return pltpu.make_async_remote_copy(
            src_ref=rows, dst_ref=rows, send_sem=g_send, recv_sem=g_recv,
            device_id=(lax.rem(me + step, device_count), head), device_id_type=MESH,
        )

    def total_copy(step):
        return pltpu.make_async_remote_copy(
            src_ref=gath.at[me, slots], dst_ref=tots.at[me],
            send_sem=t_send, recv_sem=t_recv,
            device_id=(lax.rem(me + step, device_count), other), device_id_type=MESH,
        )

    queries = lax.broadcasted_iota(jnp.int32, (1, half), 1) + head * half
    totalv[...] = jnp.zeros_like(totalv)

    def reduce_slot(slot):
        exchange(slot).wait_recv()
        length = lens[me * slots + slot]
        difference = own[slot] + recv[slot]
        keys = lax.broadcasted_iota(jnp.int32, (tokens, half), 0)
        squares = jnp.where(keys < length, difference * difference, 0.0)
        sums = jnp.sum(squares, axis=0, keepdims=True)
        sums = jnp.where(queries < length, sums * (t_scale * t_scale), 0.0)
        gath[me, slot] = sums / length.astype(jnp.float32)
        totalv[...] += sums / total_sq.astype(jnp.float32)

    hidden_copy = pltpu.make_async_remote_copy(
        src_ref=hpart.at[pl.ds(other * slots, slots)], dst_ref=hrecv,
        send_sem=h_send, recv_sem=h_recv,
        device_id=(me, other), device_id_type=MESH,
    )
    pltpu.make_async_copy(pj, pjv, pj_sem).wait()
    lag = min(2, slots)
    lanes = lax.broadcasted_iota(jnp.int32, (1, tokens), 1)

    @pl.loop(0, slots)
    def _(slot):
        for index, (source, target) in enumerate(hidden):
            fetch(4 + index, source, target, slot).wait()
        projected = lax.dot_general(
            shv[slot], pjv[...], TN, preferred_element_type=jnp.float32
        )
        errors = projected - thv[slot].astype(jnp.float32)
        squares = errors * errors
        folded = squares[:, :128]
        for start in range(128, squares.shape[1], 128):
            folded = folded + squares[:, start : start + 128]
        sums = jnp.sum(folded.T, axis=0, keepdims=True)
        sums = jnp.where(lanes < lens[me * slots + slot], sums, 0.0)
        hpart[2 * slot] = sums[:, :half]
        hpart[2 * slot + 1] = sums[:, half:]
        totalv[...] += (sums[:, :half] + sums[:, half:]) / (width * total.astype(jnp.float32))

        @pl.when(slot >= lag)
        def _():
            reduce_slot(slot - lag)

    hidden_copy.start()

    @pl.loop(slots - lag, slots)
    def _(slot):
        reduce_slot(slot)

    gath[me, slots] = totalv[...]

    @pl.loop(1, device_count)
    def _(step):
        rows_copy(step).start()
        total_copy(step).start()

    total_copy(0).start()
    hidden_copy.wait_recv()
    for row in range(slots):
        value = (hpart[head * slots + row] + hrecv[row]) / width
        for part in range(half // 128):
            index = row * (half // 128) + part
            hid_out[index : index + 1, :] = value[:, part * 128 : (part + 1) * 128]


    others = gath.at[pl.ds(0, device_count - 1)]
    pltpu.make_async_copy(others, others, g_recv).wait()
    pltpu.make_async_copy(tots, tots, t_recv).wait()
    for slot, (device, place) in enumerate(owners):
        row_out[slot] = gath[device, place]
    pieces = jnp.sum(gath[:, slots], axis=0) + jnp.sum(tots[...], axis=0)
    loss_out[...] = jnp.sum(pieces, axis=1, keepdims=True)

    hidden_copy.wait_send()
    pltpu.make_async_copy(send, send, x_send).wait()
    pltpu.make_async_copy(others, others, g_send).wait()
    pltpu.make_async_copy(tots, tots, t_send).wait()


def hand_on(hid_in, row_in, loss_in, hid_out, row_out, loss_out):
    hid_out[...] = hid_in[...]
    row_out[...] = row_in[...]
    loss_out[...] = loss_in[...]


def body(device_count, width, *operands):
    teacher_hidden, student_hidden, projector, tq, tk, student_queries, sk, lengths, plan = operands
    slots = lengths.shape[0] // device_count
    tokens = teacher_hidden.shape[0] // slots
    half = tokens // 2
    cols_t = teacher_hidden.shape[1]
    cols_h = student_hidden.shape[1]
    cols_s = student_queries.shape[1]
    bf16, f32 = jnp.bfloat16, jnp.float32
    dma = pltpu.SemaphoreType.DMA
    anywhere = pl.BlockSpec(memory_space=pl.ANY)
    vmem = pl.BlockSpec(memory_space=pltpu.VMEM)
    hidden_row, row_loss, loss = pl.pallas_call(
        functools.partial(kernel, device_count, slots, plan.shape[0], width),
        out_shape=(
            jax.ShapeDtypeStruct((slots * half // 128, 128), f32),
            jax.ShapeDtypeStruct((slots, 1, half), f32),
            jax.ShapeDtypeStruct((1, 1), f32),
        ),
        in_specs=[anywhere] * 9,
        out_specs=(vmem, vmem, vmem),
        scratch_shapes=[
            pltpu.VMEM((slots, tokens, cols_t), bf16),
            pltpu.VMEM((slots, cols_h, tokens), bf16),
            pltpu.VMEM(projector.shape, bf16),
            pltpu.VMEM((slots, tokens, cols_t), bf16),
            pltpu.VMEM((slots, tokens, cols_t), bf16),
            pltpu.VMEM((slots, cols_s, tokens), bf16),
            pltpu.VMEM((slots, cols_s, tokens), bf16),
            pltpu.SMEM(lengths.shape, jnp.int32),
            pltpu.SMEM(plan.shape, jnp.int32),
            pltpu.VMEM((1, half), f32),
            pltpu.VMEM((slots, tokens, half), f32),
            pltpu.VMEM((slots, tokens, half), f32),
            pltpu.VMEM((slots, tokens, half), f32),
            pltpu.VMEM((2 * slots, 1, half), f32),
            pltpu.VMEM((slots, 1, half), f32),
            pltpu.VMEM((device_count, slots + 1, 1, half), f32),
            pltpu.VMEM((device_count, 1, half), f32),
            dma((6, slots)),
            dma,
            dma,
            dma((slots,)),
            dma,
            dma,
            dma,
            dma,
            dma,
            dma,
            dma((2,)),
        ],
        compiler_params=pltpu.CompilerParams(
            collective_id=0, has_side_effects=True, vmem_limit_bytes=60 * 1024 * 1024
        ),
    )(
        teacher_hidden, student_hidden.T, projector, tq, tk,
        student_queries.T, sk.T, lengths, plan,
    )
    hidden_row, row_loss, loss = pl.pallas_call(
        hand_on,
        out_shape=tuple(jax.ShapeDtypeStruct(x.shape, f32) for x in (hidden_row, row_loss, loss)),
        in_specs=(vmem, vmem, vmem),
        out_specs=(vmem, vmem, vmem),
    )(hidden_row, row_loss, loss)
    return (
        hidden_row.reshape(slots * half),
        row_loss.reshape(1, 1, slots, half),
        loss.reshape(()),
    )


def solution(mesh):
    placed = (
        P("dp", "head"),
        P("dp", None),
        P(None, "head"),
        P("dp", "head"),
        P("dp", "head"),
        P("dp", "head"),
        P("dp", "head"),
        P(),
        P(),
    )

    def whole(*operands):
        width = operands[0].shape[1]
        return jax.shard_map(
            functools.partial(body, mesh.shape["dp"], width),
            mesh=mesh,
            in_specs=placed,
            out_specs=(P(("dp", "head")), P("dp", "head", None, None), P()),
            check_vma=False,
        )(*operands)

    return whole
```
